256 devices in a mesh: row: 16 (over y_hi, z), col: 16 (over x, y_lo, core).
Axes of the slice: x: 4, y: 4 (y_hi: 2, y_lo: 2; y = y_hi * 2 + y_lo), z: 8, core: 2. Of those that a mesh axis runs over, the one named last changes fastest.
Arguments:
- interior_factor: float32 [16, 16, 1, 384, 384], P('row', 'col'), as said below
- coupling_in: bfloat16 [16, 16, 1, 384, 2048], P('row', 'col'), may hold values from -1.5 to 1.5
- coupling_back: bfloat16 [16, 16, 1, 384, 2048], P('row', 'col'), may hold values from -1.5 to 1.5
- interface_block: bfloat16 [16, 16, 1, 2048, 2048], P('row', 'col'), may hold values from -6 to 6
- gran_count: int32 [16, 16, 1], replicated, may hold values from 2 to 16, as said below
- gran_index: int32 [16, 16, 1, 16], replicated, may hold values from 0 to 15, as said below
Outputs:
- schur: float32 [16, 3, 1024, 1024], P('row', None, 'col')
The draws below stay inside these ranges and needn't reach their ends.
Inputs may be any that keep to these rules, and one draw needn't show every extreme that they name: `gran_count`: each entry is an even number of granules; in every row group some subdomain has 16. `gran_index`: each row is an order of the 16 window granules, each once; window granule p of row group r is global granule 8 * r + p modulo 8 * 16; the first gran_count entries are the subdomain's interface granules. `interior_factor`: lower triangular with a positive diagonal.
All inputs are finite; a program needn't handle non-finite values.
Results may differ from the reference program's by a relative error of at most 0.0003.
Values may be sent and summed in bfloat16 or wider, within the bound.
A program may use at most 128 MiB of HBM per device.

```python
import math
import jax
import jax.numpy as jnp
from jax import lax

NI = 384
SUB_DEV = 1
WING = 16
GMAX = 2048
N_ROW = 16
N_COL = 16


def draw_interior_factor(key, part):
    first, second = jax.random.split(key)
    shape = (N_ROW, N_COL, SUB_DEV, NI, NI)
    diagonal = jax.random.uniform(first, shape[:-1], jnp.float32, 1.5, 3.0)
    spread = jax.random.normal(second, shape, jnp.float32) * (0.5 / math.sqrt(NI))
    return jnp.tril(spread, -1) + diagonal[..., None] * jnp.eye(NI, dtype=jnp.float32)


def draw_gran_count(key, part):
    first, second, third = jax.random.split(jax.random.fold_in(key, 11), 3)
    shape = (N_ROW, N_COL, SUB_DEV)
    factor_one = jax.random.randint(first, shape, 0, 4)
    factor_two = jax.random.randint(second, shape, 0, 4)
    blocks = 1 + factor_one * factor_two // 3
    chosen = jax.random.randint(third, (N_ROW,), 0, N_COL)
    columns = jnp.arange(N_COL, dtype=jnp.int32)
    subs = jnp.arange(SUB_DEV, dtype=jnp.int32)
    forced = (columns[None, :, None] == chosen[:, None, None]) & (subs[None, None, :] == 0)
    blocks = jnp.where(forced, WING // 2, blocks)
    return (2 * blocks).astype(jnp.int32)


def draw_gran_index(key, part):
    scores = jax.random.randint(jax.random.fold_in(key, 23), (N_ROW, N_COL, SUB_DEV, WING), 0, 1 << 20)
    scored = scores * WING + jnp.arange(WING, dtype=jnp.int32)
    return jnp.argsort(scored, axis=-1, stable=True).astype(jnp.int32)


def level_of(key, shape, cuts, low, largest):
    factor_of = 1.0
    for axis_at, parts in cuts:
        draws = jax.random.uniform(jax.random.fold_in(jax.random.fold_in(key, 6), axis_at), (parts,), jnp.float32, low / len(cuts), largest / len(cuts))
        factor_of = factor_of * jnp.repeat(jnp.exp(draws), shape[axis_at] // parts).reshape((-1,) + (1,) * (len(shape) - 1 - axis_at))
    return factor_of


def scatter_about(key, dims, scale, reach, cuts=(), held_as=jnp.bfloat16):
    values = scale * jax.random.normal(key, dims, jnp.float32)
    if cuts:
        values = values * level_of(key, dims, cuts, -0.22, 0.18)
    return jnp.clip(values, -reach, reach).astype(held_as)


def setup_inputs(seed: int = 0) -> dict:
    streams_of = jax.random.split(jax.random.key(seed), 7)
    interior_factor = draw_interior_factor(jax.random.fold_in(streams_of[6], 71), 0)
    coupling_in = scatter_about(streams_of[1], (N_ROW, N_COL, SUB_DEV, NI, GMAX), 0.25, 1.5, ((0, 16), (1, 16)))
    coupling_back = scatter_about(streams_of[2], (N_ROW, N_COL, SUB_DEV, NI, GMAX), 0.25, 1.5, ((0, 16), (1, 16)))
    interface_block = scatter_about(streams_of[3], (N_ROW, N_COL, SUB_DEV, GMAX, GMAX), 1.0, 6.0, ((0, 16), (1, 16)))
    gran_count = draw_gran_count(jax.random.fold_in(streams_of[6], 71), 0)
    gran_index = draw_gran_index(jax.random.fold_in(streams_of[6], 71), 0)
    return dict(interior_factor=interior_factor, coupling_in=coupling_in, coupling_back=coupling_back, interface_block=interface_block, gran_count=gran_count, gran_index=gran_index)


def select_table(count, index):
    slots = jnp.arange(index.shape[0], dtype=jnp.int32)
    live = (slots < count).astype(jnp.float32)
    return (index[:, None] == slots[None, :]).astype(jnp.float32) * live[:, None]

def place(local, table):
    wing = table.shape[0]
    width = local.shape[0]
    granule = width // wing
    blocks = local.reshape(wing, granule, wing, granule)
    moved = jnp.einsum('ap,aibj,bq->piqj', table, blocks, table, precision=lax.Precision.HIGHEST)
    return moved.reshape(width, width)

def contribution(factor, coupling_in, coupling_back, interface_block, count, index):
    solved_in = lax.linalg.triangular_solve(factor, coupling_in.astype(jnp.float32), left_side=True, lower=True).astype(jnp.bfloat16)
    solved_back = lax.linalg.triangular_solve(factor, coupling_back.astype(jnp.float32), left_side=True, lower=True).astype(jnp.bfloat16)
    product = jnp.dot(solved_back.astype(jnp.float32).T, solved_in.astype(jnp.float32), precision=lax.Precision.HIGHEST)
    local = interface_block.astype(jnp.float32) - product
    return place(local, select_table(count, index))

def reference(interior_factor, coupling_in, coupling_back, interface_block, gran_count, gran_index):
    width = coupling_in.shape[-1]
    half = width // 2

    def group_window(pieces):
        factor, inner, back, own_block, counts, index = pieces
        factor = factor.reshape((-1,) + factor.shape[-2:])
        inner = inner.reshape((-1,) + inner.shape[-2:])
        back = back.reshape((-1,) + back.shape[-2:])
        own_block = own_block.reshape((-1,) + own_block.shape[-2:])
        counts = counts.reshape(-1)
        index = index.reshape((-1, index.shape[-1]))

        def accumulate(total, item):
            return (total + contribution(*item), None)
        total, unused = lax.scan(accumulate, jnp.zeros((width, width), jnp.float32), (factor, inner, back, own_block, counts, index))
        return total
    windows = lax.map(group_window, (interior_factor, coupling_in, coupling_back, interface_block, gran_count, gran_index))
    earlier = jnp.roll(windows, 1, axis=0)
    diagonal = windows[:, :half, :half] + earlier[:, half:, half:]
    return jnp.stack([diagonal, windows[:, :half, half:], windows[:, half:, :half]], axis=1)
```

```python
import functools

import jax
import jax.numpy as jnp
from jax import lax
from jax.experimental import pallas as pl
from jax.experimental.pallas import tpu as pltpu
from jax.sharding import Mesh
from jax.sharding import PartitionSpec as P

MESH = pl.DeviceIdType.MESH
X, Y, CORE = "col_0", "col_1", "col_2"
COL = (X, Y, CORE)
NX = 4
G = 128
HEAD = 16
HIGHEST = lax.Precision.HIGHEST

B_UNITS = ["b1p", "b1m", "b2op", "b2om", "b2sp", "b2sm", "b3"]
A_UNITS = ["a1_2", "a1_1", "a1_3", "a1_0", "a2p", "a2m", "a3op", "a3om", "a3sp", "a3sm"]


def unit_numbers():
    names = []
    for block in (3, 1):
        names += [(block, u) for u in B_UNITS]
    for block in (2, 0):
        names += [(block, u) for u in A_UNITS]
    names.append((3, "carry"))
    return {name: i for i, name in enumerate(names)}


UNIT = unit_numbers()


def mm(a, b):
    return jnp.dot(a, b, precision=HIGHEST, preferred_element_type=jnp.float32)


def inverse_of_block(block):
    n = block.shape[0]
    row = lax.broadcasted_iota(jnp.int32, (n, n), 0)
    col = lax.broadcasted_iota(jnp.int32, (n, n), 1)
    diagonal = jnp.where(row == col, block, 0.0)
    down = 1.0 / jnp.sum(diagonal, axis=1, keepdims=True)
    across = 1.0 / jnp.sum(diagonal, axis=0, keepdims=True)

    def below(size):
        return (
            (row // (2 * size) == col // (2 * size))
            & ((row // size) % 2 == 1)
            & ((col // size) % 2 == 0)
        )

    found = jnp.where(row == col, down, 0.0) - jnp.where(below(1), block, 0.0) * down * across
    size = 2
    while size < n:
        part = jnp.where(below(size), block, 0.0)
        found = found - mm(mm(found, part), found)
        size *= 2
    return found


def kernel(
    tab, live, factor_hbm, in_hbm, back_hbm, own_hbm, out,
    factor, ci, cb, ibo, ibp, w, in_o, in_p, bt, bp, acc, sendb, recvb,
    factor_sem, load_sem, swap_send, swap_recv, send_sem, recv_sem,
):
    row = lax.axis_index("row")
    rows = lax.axis_size("row")
    x = lax.axis_index(X)
    y = lax.axis_index(Y)
    k = lax.axis_index(CORE)
    plus = {X: lax.rem(x + 1, NX)}
    minus = {X: lax.rem(x + NX - 1, NX)}
    over = {Y: 1 - y}
    mate = {CORE: 1 - k}
    after = {"row": lax.rem(row + 1, rows)}
    before = {"row": lax.rem(row + rows - 1, rows)}

    barrier = pltpu.get_barrier_semaphore()
    for to in (mate, plus, minus, over, after, before):
        pl.semaphore_signal(barrier, inc=1, device_id=to, device_id_type=MESH)

    def load_columns(src, dst, q, which):
        return pltpu.make_async_copy(
            src.at[:, pl.ds(q * G, G)], dst.at[q], load_sem.at[which, q]
        )

    loads = [
        [pltpu.make_async_copy(factor_hbm, factor, factor_sem)],
        [load_columns(back_hbm, cb, q, 0) for q in range(16)],
        [load_columns(in_hbm, ci, q, 1) for q in range(16)],
        [
            pltpu.make_async_copy(
                own_hbm.at[:, k, :, pl.ds(q * G, G)], ibo.at[q], load_sem.at[2, q]
            )
            for q in range(16)
        ],
    ]
    for load in loads:
        for copy in load:
            copy.start()

    def wait_for(load):
        for copy in load:
            copy.wait()

    pl.semaphore_wait(barrier, 6)

    def swap(src, dst, n):
        return pltpu.make_async_remote_copy(
            src_ref=src, dst_ref=dst, send_sem=swap_send.at[n], recv_sem=swap_recv.at[n],
            device_id=mate, device_id_type=MESH,
        )

    swaps = {
        "back1": swap(bt.at[pl.ds(8, 8), 1 - k], bp.at[pl.ds(8, 8)], 16),
        "back0": swap(bt.at[pl.ds(0, 8), 1 - k], bp.at[pl.ds(0, 8)], 17),
        "in1": swap(in_o.at[:, pl.ds(1024, 1024)], in_p.at[:, pl.ds(1024, 1024)], 18),
        "in0": swap(in_o.at[:, pl.ds(0, 1024)], in_p.at[:, pl.ds(0, 1024)], 19),
    }
    for q in range(16):
        swaps[q] = swap(own_hbm.at[:, 1 - k, :, pl.ds(q * G, G)], ibp.at[q], q)
        swaps[q].start()

    wait_for(loads[0])
    n = factor.shape[0]

    def part(i, j):
        return factor[i * G : (i + 1) * G, j * G : (j + 1) * G]

    x0, x1, x2 = (inverse_of_block(part(i, i)) for i in range(3))
    x10 = -mm(mm(x1, part(1, 0)), x0)
    t0 = mm(x2, part(2, 0))
    t1 = mm(x2, part(2, 1))
    x20 = -(mm(t0, x0) + mm(t1, x10))
    x21 = -mm(t1, x1)
    zero = jnp.zeros((G, G), jnp.float32)
    for i, line in enumerate(((x0, zero, zero), (x10, x1, zero), (x20, x21, x2))):
        for j, piece in enumerate(line):
            high = piece.astype(jnp.bfloat16)
            w[i * G : (i + 1) * G, j * G : (j + 1) * G] = high
            w[i * G : (i + 1) * G, n + j * G : n + (j + 1) * G] = (
                piece - high.astype(jnp.float32)
            ).astype(jnp.bfloat16)

    def window_granule(h, j):
        return h * 8 + 2 * lax.rem(x + j // 2, NX) + lax.rem(j + y, 2)

    def granule_of(ref, p):
        a = tab[0, p]
        piece = ref[a]
        return piece * jnp.full(piece.shape, live[0, p]).astype(piece.dtype)

    def solve_back(h):
        def body(pair, _):
            pieces = [granule_of(cb, window_granule(h, 2 * pair + i)) for i in (0, 1)]
            both = jnp.concatenate(pieces, axis=1)
            twice = jnp.concatenate([both, both], axis=0)
            solved = lax.dot_general(
                twice, w[...], (((0,), (1,)), ((), ())), preferred_element_type=jnp.float32
            ).astype(jnp.bfloat16)
            bt[pl.ds(h * 8 + 2 * pair, 2)] = solved.reshape(2, 2, 64, n)
            return 0

        lax.fori_loop(0, 4, body, 0)

    def solve_in(half):
        def body(pair, _):
            p = half * 8 + 2 * pair
            both = jnp.concatenate([granule_of(ci, p), granule_of(ci, p + 1)], axis=1)
            twice = jnp.concatenate([both, both], axis=0)
            solved = jnp.dot(w[...], twice, preferred_element_type=jnp.float32)
            in_o[:, pl.ds(pl.multiple_of(p * G, 2 * G), 2 * G)] = solved.astype(jnp.bfloat16)
            return 0

        lax.fori_loop(0, 4, body, 0)

    wait_for(loads[1])
    solve_back(1)
    swaps["back1"].start()
    wait_for(loads[2])
    solve_in(1)
    swaps["in1"].start()
    solve_in(0)
    swaps["in0"].start()

    def product(block):
        h, half = block // 2, block % 2
        lhs = jnp.concatenate(
            [bt[pl.ds(h * 8, 8), k].reshape(512, n), bp[pl.ds(h * 8, 8)].reshape(512, n)], axis=1
        )

        def body(pair, _):
            p = half * 8 + 2 * pair
            at = pl.ds(pl.multiple_of(p * G, 2 * G), 2 * G)
            rhs = jnp.concatenate([in_o[:, at], in_p[:, at]], axis=0)
            made = jnp.dot(lhs, rhs, preferred_element_type=jnp.float32)
            for j in range(8):
                g = window_granule(h, j)
                for i in (0, 1):
                    total = -made[j * 64 : (j + 1) * 64, i * G : (i + 1) * G]
                    for ref, which in ((ibo, 0), (ibp, 1)):
                        at_row, at_col = tab[which, g], tab[which, p + i]
                        both = live[which, g] * live[which, p + i]
                        tile = ref[at_col, at_row]
                        total = total + both * tile.astype(jnp.float32)
                    acc[block, j, 2 * pair + i] = total
            return 0

        lax.fori_loop(0, 4, body, 0)

    def copy_of(block, name, tiles, to):
        u = UNIT[block, name]
        size = pl.ds(0, HEAD + 64 * tiles)
        return pltpu.make_async_remote_copy(
            src_ref=sendb.at[u, size], dst_ref=recvb.at[u, size],
            send_sem=send_sem.at[u], recv_sem=recv_sem.at[u],
            device_id=to, device_id_type=MESH,
        )

    copies = []

    def send(block, name, slots, first, last, to):
        u = UNIT[block, name]
        wide = last - first
        most = jnp.full((HEAD, G), 1e-30, jnp.float32)
        for j in slots:
            seen = jnp.abs(acc[block, j, first:last]).reshape(wide * 4, HEAD, G)
            most = jnp.maximum(most, jnp.max(seen, axis=0))
        power = jnp.ceil(jnp.log2(most) + 0.015)
        scale = jnp.exp2(15.0 - power)
        sendb[u, 0:HEAD] = power.astype(jnp.int32).astype(jnp.int16)
        at = HEAD
        for j in slots:
            codes = acc[block, j, first:last].reshape(wide * 4, HEAD, G) * scale[None]
            codes = jnp.round(codes).astype(jnp.int32).astype(jnp.int16)
            sendb[u, at : at + 64 * wide] = codes.reshape(64 * wide, G)
            at += 64 * wide
        copy = copy_of(block, name, len(slots) * wide, to)
        copy.start()
        copies.append(copy)

    def take(block, name, slots, first, last, to, onto=None):
        u = UNIT[block, name]
        wide = last - first
        copy_of(block, name, len(slots) * wide, to).wait_recv()
        scale = jnp.exp2(recvb[u, 0:HEAD].astype(jnp.float32) - 15.0)
        at = HEAD
        onto = block if onto is None else onto
        for j in slots:
            got = recvb[u, at : at + 64 * wide].astype(jnp.float32).reshape(wide * 4, HEAD, G)
            got = (got * scale[None]).reshape(wide, 64, G)
            acc[onto, j, first:last] = acc[onto, j, first:last] + got
            at += 64 * wide

    def b_first(block):
        send(block, "b1p", (4, 5), 0, 4, plus)
        send(block, "b1m", (4, 5), 4, 8, minus)
        send(block, "b2op", (2, 3), 4, 8, plus)
        send(block, "b2om", (6, 7), 0, 4, minus)

    def b_second(block):
        take(block, "b1p", (2, 3), 0, 4, plus)
        send(block, "b2sp", (2, 3), 0, 4, plus)
        take(block, "b1m", (6, 7), 4, 8, minus)
        send(block, "b2sm", (6, 7), 4, 8, minus)

    def b_third(block):
        take(block, "b2op", (0, 1), 4, 8, plus)
        take(block, "b2om", (0, 1), 0, 4, minus)
        take(block, "b2sp", (0, 1), 0, 4, plus)
        take(block, "b2sm", (0, 1), 4, 8, minus)
        send(block, "b3", (1,), 0, 8, over)

    def b_last(block):
        take(block, "b3", (0,), 0, 8, over)

    def a_first(block):
        for d in (2, 1, 3, 0):
            send(block, f"a1_{d}", (2 * d + 1,), 0, 8, over)

    def a_second(block):
        take(block, "a1_2", (4,), 0, 8, over)
        send(block, "a2p", (4,), 0, 4, plus)
        send(block, "a2m", (4,), 4, 8, minus)
        take(block, "a1_1", (2,), 0, 8, over)
        send(block, "a3op", (2,), 4, 8, plus)
        take(block, "a1_3", (6,), 0, 8, over)
        send(block, "a3om", (6,), 0, 4, minus)

    def a_third(block):
        take(block, "a2p", (2,), 0, 4, plus)
        send(block, "a3sp", (2,), 0, 4, plus)
        take(block, "a2m", (6,), 4, 8, minus)
        send(block, "a3sm", (6,), 4, 8, minus)
        take(block, "a1_0", (0,), 0, 8, over)

    def a_last(block):
        take(block, "a3op", (0,), 4, 8, plus)
        take(block, "a3om", (0,), 0, 4, minus)
        take(block, "a3sp", (0,), 0, 4, plus)
        take(block, "a3sm", (0,), 4, 8, minus)

    def emit(block):
        for q in range(8):
            out[block, :, q * G : (q + 1) * G] = acc[block, 0, q]

    wait_for(loads[3])
    for q in range(16):
        swaps[q].wait_recv()
    swaps["back1"].wait_recv()
    swaps["in1"].wait_recv()
    product(3)
    b_first(3)
    swaps["in0"].wait_recv()
    product(2)
    a_first(2)
    solve_back(0)
    swaps["back0"].start()
    b_second(3)
    swaps["back0"].wait_recv()
    product(1)
    b_first(1)
    b_third(3)
    product(0)
    a_first(0)
    b_second(1)
    b_last(3)
    send(3, "carry", (0,), 0, 8, after)
    a_second(2)
    b_third(1)
    a_third(2)
    a_second(0)
    a_last(2)
    emit(2)
    a_third(0)
    b_last(1)
    emit(1)
    take(3, "carry", (0,), 0, 8, after, onto=0)
    a_last(0)
    emit(0)

    for copy in swaps.values():
        copy.wait_send()
    for copy in copies:
        copy.wait_send()


def tables(gran_count, gran_index):
    row = lax.axis_index("row")
    chip = lax.axis_index((X, Y))
    k = lax.axis_index(CORE)
    counts = lax.dynamic_slice(gran_count, (row, 2 * chip, 0), (1, 2, 1))[0]
    index = lax.dynamic_slice(gran_index, (row, 2 * chip, 0, 0), (1, 2, 1, gran_index.shape[-1]))[0, :, 0]
    slots = jnp.arange(index.shape[1], dtype=jnp.int32)
    place = jnp.sum(jnp.where(index[:, :, None] == slots[None, None, :], slots[None, :, None], 0), axis=1)
    live = (place < counts).astype(jnp.float32)
    place = jnp.where(k == 0, place, place[::-1])
    live = jnp.where(k == 0, live, live[::-1])
    return place, live


def on_device(interior_factor, coupling_in, coupling_back, interface_block, gran_count, gran_index):
    factor = interior_factor[0, 0, 0]
    inner = coupling_in[0, 0, 0]
    back = coupling_back[0, 0, 0]
    n, width = inner.shape
    own = interface_block[0, 0, 0].reshape(16, 2, 64, width)
    units = len(UNIT)
    size = HEAD + 64 * 8
    hbm = pl.BlockSpec(memory_space=pl.ANY)
    out = pl.pallas_call(
        kernel,
        out_shape=jax.ShapeDtypeStruct((3, 64, width // 2), jnp.float32),
        in_specs=[pl.BlockSpec(memory_space=pltpu.SMEM)] * 2 + [hbm, hbm, hbm, hbm],
        out_specs=pl.BlockSpec(memory_space=pltpu.VMEM),
        scratch_shapes=[
            pltpu.VMEM((n, n), jnp.float32),
            pltpu.VMEM((16, n, G), jnp.bfloat16),
            pltpu.VMEM((16, n, G), jnp.bfloat16),
            pltpu.VMEM((16, 16, 64, G), jnp.bfloat16),
            pltpu.VMEM((16, 16, 64, G), jnp.bfloat16),
            pltpu.VMEM((n, 2 * n), jnp.bfloat16),
            pltpu.VMEM((n, width), jnp.bfloat16),
            pltpu.VMEM((n, width), jnp.bfloat16),
            pltpu.VMEM((16, 2, 64, n), jnp.bfloat16),
            pltpu.VMEM((16, 64, n), jnp.bfloat16),
            pltpu.VMEM((4, 8, 8, 64, G), jnp.float32),
            pltpu.VMEM((units, size, G), jnp.int16),
            pltpu.VMEM((units, size, G), jnp.int16),
            pltpu.SemaphoreType.DMA,
            pltpu.SemaphoreType.DMA((3, 16)),
            pltpu.SemaphoreType.DMA((20,)),
            pltpu.SemaphoreType.DMA((20,)),
            pltpu.SemaphoreType.DMA((units,)),
            pltpu.SemaphoreType.DMA((units,)),
        ],
        compiler_params=pltpu.CompilerParams(
            collective_id=0, has_side_effects=True, vmem_limit_bytes=56 * 1024 * 1024
        ),
    )(*tables(gran_count, gran_index), factor, inner, back, own)
    return out[None]


def solution(mesh):
    split = Mesh(mesh.devices.reshape(mesh.shape["row"], 4, 2, 2), ("row", X, Y, CORE))
    spec = P("row", COL, None, None, None)
    return jax.shard_map(
        on_device,
        mesh=split,
        in_specs=(spec, spec, spec, spec, P(), P()),
        out_specs=P("row", None, COL, None),
        check_vma=False,
    )
```

```python
import functools

import jax
import jax.numpy as jnp
from jax import lax
from jax.experimental import pallas as pl
from jax.experimental.pallas import tpu as pltpu
from jax.sharding import Mesh
from jax.sharding import PartitionSpec as P

MESH = pl.DeviceIdType.MESH
X, Y, CORE = "col_0", "col_1", "col_2"
COL = (X, Y, CORE)
NX = 4
G = 128
HEAD = 16
HIGHEST = lax.Precision.HIGHEST

Y_FIRST = 7
B_UNITS = ["b1p", "b1m", "b2op", "b2om", "b2sp", "b2sm", "b3"]
A_UNITS = ["a1_2", "a1_1", "a1_3", "a1_0", "a2p", "a2m", "a3op", "a3om", "a3sp", "a3sm"]


def unit_numbers():
    names = [(h, u) for h in (1, 0) for u in B_UNITS + A_UNITS] + [(1, "carry")]
    return {name: i for i, name in enumerate(names)}


UNIT = unit_numbers()


def mm(a, b):
    return jnp.dot(a, b, precision=HIGHEST, preferred_element_type=jnp.float32)


def inverses_of_blocks(blocks):
    n = blocks[0].shape[0]
    row = lax.broadcasted_iota(jnp.int32, (n, n), 0)
    col = lax.broadcasted_iota(jnp.int32, (n, n), 1)

    def below(shift):
        upper, lower = row >> shift, col >> shift
        return ((upper & 1) == 1) & (upper == lower + 1)

    found = []
    for block in blocks:
        diagonal = jnp.where(row == col, block, 0.0)
        down = 1.0 / jnp.sum(diagonal, axis=1, keepdims=True)
        across = 1.0 / jnp.sum(diagonal, axis=0, keepdims=True)
        under = jnp.where(below(0), block, 0.0)
        found.append(jnp.where(row == col, down, 0.0) - under * down * across)
    for shift in range(1, 7):
        mask = below(shift)
        lines = [mm(f, jnp.where(mask, block, 0.0)) for f, block in zip(found, blocks)]
        found = [f - mm(line, f) for f, line in zip(found, lines)]
    return found


def kernel(
    count_hbm, index_hbm, factor_hbm, in_hbm, back_hbm, own_hbm, out,
    counts, index, tab, live, factor, ci, cb, ibo, ibs, ibp, w, in_o, in_p, bt, bp, acc, sendb, recvb,
    factor_sem, load_sem, swap_send, swap_recv, send_sem, recv_sem,
):
    row = lax.axis_index("row")
    rows = lax.axis_size("row")
    x = lax.axis_index(X)
    y = lax.axis_index(Y)
    k = lax.axis_index(CORE)
    plus = {X: lax.rem(x + 1, NX)}
    minus = {X: lax.rem(x + NX - 1, NX)}
    over = {Y: 1 - y}
    mate = {CORE: 1 - k}
    after = {"row": lax.rem(row + 1, rows)}
    before = {"row": lax.rem(row + rows - 1, rows)}

    barrier = pltpu.get_barrier_semaphore()
    for to in (mate, plus, minus, over, after, before):
        pl.semaphore_signal(barrier, inc=1, device_id=to, device_id_type=MESH)

    def load_columns(src, dst, q, which):
        return pltpu.make_async_copy(
            src.at[:, pl.ds(q * G, G)], dst.at[q], load_sem.at[which, q]
        )

    loads = [
        [pltpu.make_async_copy(factor_hbm, factor, factor_sem)],
        [load_columns(back_hbm, cb, q, 0) for q in range(16)],
        [load_columns(in_hbm, ci, q, 1) for q in range(16)],
        [
            pltpu.make_async_copy(
                own_hbm.at[:, :, :, pl.ds(q * G, G)], ibo.at[q], load_sem.at[2, q]
            )
            for q in range(16)
        ],
    ]
    mine = 4 * x + 2 * y + k
    loads[0] += [
        pltpu.make_async_copy(count_hbm.at[row], counts, load_sem.at[3, 0]),
        pltpu.make_async_copy(index_hbm.at[row, mine], index, load_sem.at[3, 1]),
    ]
    def start(load):
        for copy in load:
            copy.start()

    def wait_for(load):
        for copy in load:
            copy.wait()

    start(loads[0])

    def swap(src, dst, n):
        return pltpu.make_async_remote_copy(
            src_ref=src, dst_ref=dst, send_sem=swap_send.at[n], recv_sem=swap_recv.at[n],
            device_id=mate, device_id_type=MESH,
        )

    swaps = {
        "back1": swap(bt.at[pl.ds(8, 8), 1 - k], bp.at[pl.ds(8, 8)], 4),
        "back0": swap(bt.at[pl.ds(0, 8), 1 - k], bp.at[pl.ds(0, 8)], 5),
        "in1": swap(in_o.at[:, pl.ds(1024, 1024)], in_p.at[:, pl.ds(1024, 1024)], 6),
        "in0": swap(in_o.at[:, pl.ds(0, 1024)], in_p.at[:, pl.ds(0, 1024)], 7),
    }
    for block in range(4):
        swaps[block] = swap(ibs.at[block], ibp.at[block], block)

    wait_for(loads[0])
    for load in (loads[3], loads[1], loads[2]):
        start(load)
    n = factor.shape[0]
    at = [index[0, a] for a in range(16)]
    count = counts[mine]
    for p in range(16):
        place = jnp.int32(0)
        for a in range(1, 16):
            place = place + jnp.where(at[a] == p, a, 0)
        tab[0, p] = place & 15
        live[0, p] = jnp.where(place < count, 1.0, 0.0)

    def part(i, j):
        return factor[i * G : (i + 1) * G, j * G : (j + 1) * G]

    x0, x1, x2 = inverses_of_blocks([part(i, i) for i in range(3)])
    x10 = -mm(mm(x1, part(1, 0)), x0)
    t0 = mm(x2, part(2, 0))
    t1 = mm(x2, part(2, 1))
    x20 = -(mm(t0, x0) + mm(t1, x10))
    x21 = -mm(t1, x1)
    zero = jnp.zeros((G, G), jnp.float32)
    for i, line in enumerate(((x0, zero, zero), (x10, x1, zero), (x20, x21, x2))):
        for j, piece in enumerate(line):
            high = piece.astype(jnp.bfloat16)
            w[i * G : (i + 1) * G, j * G : (j + 1) * G] = high
            w[i * G : (i + 1) * G, n + j * G : n + (j + 1) * G] = (
                piece - high.astype(jnp.float32)
            ).astype(jnp.bfloat16)

    def window_granule(h, j):
        return h * 8 + 2 * lax.rem(x + j // 2, NX) + lax.rem(j + y, 2)

    def granule_of(ref, p):
        a = tab[0, p]
        piece = ref[a]
        return piece * jnp.full(piece.shape, live[0, p]).astype(piece.dtype)

    def solve_back(h):
        def body(pair, _):
            pieces = [granule_of(cb, window_granule(h, 2 * pair + i)) for i in (0, 1)]
            both = jnp.concatenate(pieces, axis=1)
            twice = jnp.concatenate([both, both], axis=0)
            solved = lax.dot_general(
                twice, w[...], (((0,), (1,)), ((), ())), preferred_element_type=jnp.float32
            ).astype(jnp.bfloat16)
            bt[pl.ds(h * 8 + 2 * pair, 2)] = solved.reshape(2, 2, 64, n)
            return 0

        lax.fori_loop(0, 4, body, 0)

    def solve_in(half):
        def body(pair, _):
            p = half * 8 + 2 * pair
            both = jnp.concatenate([granule_of(ci, p), granule_of(ci, p + 1)], axis=1)
            twice = jnp.concatenate([both, both], axis=0)
            solved = jnp.dot(w[...], twice, preferred_element_type=jnp.float32)
            in_o[:, pl.ds(pl.multiple_of(p * G, 2 * G), 2 * G)] = solved.astype(jnp.bfloat16)
            return 0

        lax.fori_loop(0, 4, body, 0)

    def gather(block):
        h, half = block // 2, block % 2

        def body(j, _):
            g = window_granule(h, j)
            for q in range(8):
                p = half * 8 + q
                tile = ibo[tab[0, p], tab[0, g], 1 - k]
                keep = jnp.full(tile.shape, live[0, g] * live[0, p]).astype(tile.dtype)
                ibs[block, j, q] = tile * keep
            return 0

        lax.fori_loop(0, 8, body, 0)
        swaps[block].start()

    wait_for(loads[3])
    pl.semaphore_wait(barrier, 6)
    gather(2)
    wait_for(loads[1])
    solve_back(1)
    swaps["back1"].start()
    wait_for(loads[2])
    solve_in(0)
    swaps["in0"].start()
    gather(3)
    solve_in(1)
    swaps["in1"].start()

    def product(block):
        h, half = block // 2, block % 2
        lhs = jnp.concatenate(
            [bt[pl.ds(h * 8, 8), k].reshape(512, n), bp[pl.ds(h * 8, 8)].reshape(512, n)], axis=1
        )

        def body(pair, _):
            p = half * 8 + 2 * pair
            at = pl.ds(pl.multiple_of(p * G, 2 * G), 2 * G)
            rhs = jnp.concatenate([in_o[:, at], in_p[:, at]], axis=0)
            made = jnp.dot(lhs, rhs, preferred_element_type=jnp.float32)
            for j in range(8):
                g = window_granule(h, j)
                for i in (0, 1):
                    total = -made[j * 64 : (j + 1) * 64, i * G : (i + 1) * G]
                    tile = ibo[tab[0, p + i], tab[0, g], k].astype(jnp.float32)
                    total = total + tile * (live[0, g] * live[0, p + i])
                    total = total + ibp[block, j, 2 * pair + i].astype(jnp.float32)
                    acc[h, j, p + i] = total
            return 0

        lax.fori_loop(0, 4, body, 0)

    def copy_of(block, name, tiles, to):
        u = UNIT[block, name]
        size = pl.ds(0, HEAD + 64 * tiles)
        return pltpu.make_async_remote_copy(
            src_ref=sendb.at[u, size], dst_ref=recvb.at[u, size],
            send_sem=send_sem.at[u], recv_sem=recv_sem.at[u],
            device_id=to, device_id_type=MESH,
        )

    copies = []

    def send(block, name, slots, first, last, to):
        u = UNIT[block, name]
        wide = last - first
        most = jnp.full((HEAD, G), 1e-30, jnp.float32)
        for j in slots:
            seen = jnp.abs(acc[block, j, first:last]).reshape(wide * 4, HEAD, G)
            most = jnp.maximum(most, jnp.max(seen, axis=0))
        power = jnp.ceil(jnp.log2(most) + 0.015)
        scale = jnp.exp2(15.0 - power)
        sendb[u, 0:HEAD] = power.astype(jnp.int32).astype(jnp.int16)
        at = HEAD
        for j in slots:
            codes = acc[block, j, first:last].reshape(wide * 4, HEAD, G) * scale[None]
            codes = jnp.round(codes).astype(jnp.int32).astype(jnp.int16)
            sendb[u, at : at + 64 * wide] = codes.reshape(64 * wide, G)
            at += 64 * wide
        copy = copy_of(block, name, len(slots) * wide, to)
        copy.start()
        copies.append(copy)

    def take(block, name, slots, first, last, to, onto=None):
        u = UNIT[block, name]
        wide = last - first
        copy_of(block, name, len(slots) * wide, to).wait_recv()
        scale = jnp.exp2(recvb[u, 0:HEAD].astype(jnp.float32) - 15.0)
        at = HEAD
        h, first, last = (block, first, last) if onto is None else onto
        for j in slots:
            got = recvb[u, at : at + 64 * wide].astype(jnp.float32).reshape(wide * 4, HEAD, G)
            got = (got * scale[None]).reshape(wide, 64, G)
            acc[h, j, first:last] = acc[h, j, first:last] + got
            at += 64 * wide

    a_to, b_to = Y_FIRST, 16
    a_mid = (3, 4)
    b_mid = (12, 11)

    def b_first(h):
        send(h, "b1p", (4, 5), a_to, b_mid[h], plus)
        send(h, "b1m", (4, 5), b_mid[h], b_to, minus)
        send(h, "b2op", (2, 3), b_mid[h], b_to, plus)
        send(h, "b2om", (6, 7), a_to, b_mid[h], minus)

    def b_second(h):
        take(h, "b1p", (2, 3), a_to, b_mid[h], plus)
        send(h, "b2sp", (2, 3), a_to, b_mid[h], plus)
        take(h, "b1m", (6, 7), b_mid[h], b_to, minus)
        send(h, "b2sm", (6, 7), b_mid[h], b_to, minus)

    def b_third(h):
        take(h, "b2op", (0, 1), b_mid[h], b_to, plus)
        take(h, "b2om", (0, 1), a_to, b_mid[h], minus)
        take(h, "b2sp", (0, 1), a_to, b_mid[h], plus)
        take(h, "b2sm", (0, 1), b_mid[h], b_to, minus)
        send(h, "b3", (1,), a_to, b_to, over)

    def b_last(h):
        take(h, "b3", (0,), a_to, b_to, over)

    def a_first(h):
        for d in (2, 1, 3, 0):
            send(h, f"a1_{d}", (2 * d + 1,), 0, a_to, over)

    def a_second(h):
        take(h, "a1_2", (4,), 0, a_to, over)
        send(h, "a2p", (4,), 0, a_mid[h], plus)
        send(h, "a2m", (4,), a_mid[h], a_to, minus)
        take(h, "a1_1", (2,), 0, a_to, over)
        send(h, "a3op", (2,), a_mid[h], a_to, plus)
        take(h, "a1_3", (6,), 0, a_to, over)
        send(h, "a3om", (6,), 0, a_mid[h], minus)

    def a_third(h):
        take(h, "a2p", (2,), 0, a_mid[h], plus)
        send(h, "a3sp", (2,), 0, a_mid[h], plus)
        take(h, "a2m", (6,), a_mid[h], a_to, minus)
        send(h, "a3sm", (6,), a_mid[h], a_to, minus)
        take(h, "a1_0", (0,), 0, a_to, over)

    def a_last(h):
        take(h, "a3op", (0,), a_mid[h], a_to, plus)
        take(h, "a3om", (0,), 0, a_mid[h], minus)
        take(h, "a3sp", (0,), 0, a_mid[h], plus)
        take(h, "a3sm", (0,), a_mid[h], a_to, minus)

    def emit(block):
        h, half = block // 2, block % 2
        for q in range(8):
            out[block, :, q * G : (q + 1) * G] = acc[h, 0, half * 8 + q]

    swaps[2].wait_recv()
    swaps["back1"].wait_recv()
    swaps["in0"].wait_recv()
    product(2)
    a_first(1)
    swaps["in1"].wait_recv()
    swaps[3].wait_recv()
    product(3)
    b_first(1)
    gather(0)
    solve_back(0)
    swaps["back0"].start()
    gather(1)
    b_second(1)
    swaps["back0"].wait_recv()
    swaps[0].wait_recv()
    product(0)
    a_second(1)
    b_third(1)
    a_first(0)
    swaps[1].wait_recv()
    product(1)
    b_first(0)
    a_third(1)
    b_last(1)
    send(1, "carry", (0,), 8, 16, after)
    b_second(0)
    a_second(0)
    a_last(1)
    emit(2)
    b_third(0)
    a_third(0)
    take(1, "carry", (0,), 8, 16, after, onto=(0, 0, 8))
    b_last(0)
    emit(1)
    a_last(0)
    emit(0)

    for copy in swaps.values():
        copy.wait_send()
    for copy in copies:
        copy.wait_send()


def on_device(interior_factor, coupling_in, coupling_back, interface_block, gran_count, gran_index):
    factor = interior_factor[0, 0, 0]
    inner = coupling_in[0, 0, 0]
    back = coupling_back[0, 0, 0]
    n, width = inner.shape
    own = interface_block[0, 0, 0].reshape(16, 2, 64, width)
    units = len(UNIT)
    size = HEAD + 64 * 10
    hbm = pl.BlockSpec(memory_space=pl.ANY)
    out = pl.pallas_call(
        kernel,
        out_shape=pltpu.VMEM((3, 64, width // 2), jnp.float32),
        in_specs=[hbm, hbm, hbm, hbm, hbm, hbm],
        out_specs=pl.BlockSpec(memory_space=pltpu.VMEM),
        scratch_shapes=[
            pltpu.SMEM((16,), jnp.int32),
            pltpu.SMEM((1, 16), jnp.int32),
            pltpu.SMEM((1, 16), jnp.int32),
            pltpu.SMEM((1, 16), jnp.float32),
            pltpu.VMEM((n, n), jnp.float32),
            pltpu.VMEM((16, n, G), jnp.bfloat16),
            pltpu.VMEM((16, n, G), jnp.bfloat16),
            pltpu.VMEM((16, 16, 2, 64, G), jnp.bfloat16),
            pltpu.VMEM((4, 8, 8, 64, G), jnp.bfloat16),
            pltpu.VMEM((4, 8, 8, 64, G), jnp.bfloat16),
            pltpu.VMEM((n, 2 * n), jnp.bfloat16),
            pltpu.VMEM((n, width), jnp.bfloat16),
            pltpu.VMEM((n, width), jnp.bfloat16),
            pltpu.VMEM((16, 2, 64, n), jnp.bfloat16),
            pltpu.VMEM((16, 64, n), jnp.bfloat16),
            pltpu.VMEM((2, 8, 16, 64, G), jnp.float32),
            pltpu.VMEM((units, size, G), jnp.int16),
            pltpu.VMEM((units, size, G), jnp.int16),
            pltpu.SemaphoreType.DMA,
            pltpu.SemaphoreType.DMA((4, 16)),
            pltpu.SemaphoreType.DMA((8,)),
            pltpu.SemaphoreType.DMA((8,)),
            pltpu.SemaphoreType.DMA((units,)),
            pltpu.SemaphoreType.DMA((units,)),
        ],
        compiler_params=pltpu.CompilerParams(
            collective_id=0, has_side_effects=True, vmem_limit_bytes=56 * 1024 * 1024
        ),
    )(gran_count[:, :, 0], gran_index, factor, inner, back, own)
    return out[None]


def solution(mesh):
    split = Mesh(mesh.devices.reshape(mesh.shape["row"], 4, 2, 2), ("row", X, Y, CORE))
    spec = P("row", COL, None, None, None)
    return jax.shard_map(
        on_device,
        mesh=split,
        in_specs=(spec, spec, spec, spec, P(), P()),
        out_specs=P("row", None, COL, None),
        check_vma=False,
    )
```

```python
import functools

import jax
import jax.numpy as jnp
from jax import lax
from jax.experimental import pallas as pl
from jax.experimental.pallas import tpu as pltpu
from jax.sharding import Mesh
from jax.sharding import PartitionSpec as P

MESH = pl.DeviceIdType.MESH
X, Y, CORE = "col_0", "col_1", "col_2"
COL = (X, Y, CORE)
NX = 4
G = 128
HEAD = 16
HIGHEST = lax.Precision.HIGHEST

Y_FIRST = 7
B_UNITS = ["b1p", "b1m", "b2op", "b2om", "b2sp", "b2sm", "b3"]
A_UNITS = ["a1_2", "a1_1", "a1_3", "a1_0", "a2p", "a2m", "a3op", "a3om", "a3sp", "a3sm"]


def unit_numbers():
    names = [(h, u) for h in (1, 0) for u in B_UNITS + A_UNITS] + [(1, "carry")]
    return {name: i for i, name in enumerate(names)}


UNIT = unit_numbers()


def mm(a, b):
    return jnp.dot(a, b, precision=HIGHEST, preferred_element_type=jnp.float32)


def inverses_of_blocks(blocks):
    n = blocks[0].shape[0]
    row = lax.broadcasted_iota(jnp.int32, (n, n), 0)
    col = lax.broadcasted_iota(jnp.int32, (n, n), 1)

    def below(shift):
        upper, lower = row >> shift, col >> shift
        return ((upper & 1) == 1) & (upper == lower + 1)

    found = []
    for block in blocks:
        diagonal = jnp.where(row == col, block, 0.0)
        down = 1.0 / jnp.sum(diagonal, axis=1, keepdims=True)
        across = 1.0 / jnp.sum(diagonal, axis=0, keepdims=True)
        under = jnp.where(below(0), block, 0.0)
        found.append(jnp.where(row == col, down, 0.0) - under * down * across)
    for shift in range(1, 7):
        mask = below(shift)
        lines = [mm(f, jnp.where(mask, block, 0.0)) for f, block in zip(found, blocks)]
        found = [f - mm(line, f) for f, line in zip(found, lines)]
    return found


def kernel(
    count_hbm, index_hbm, factor_hbm, in_hbm, back_hbm, own_hbm, out,
    counts, index, tab, live, factor, ci, cb, ibo, ibs, ibp, w, in_o, in_p, bt, bp, acc, sendb, recvb,
    factor_sem, load_sem, swap_send, swap_recv, send_sem, recv_sem,
):
    row = lax.axis_index("row")
    rows = lax.axis_size("row")
    x = lax.axis_index(X)
    y = lax.axis_index(Y)
    k = lax.axis_index(CORE)
    plus = {X: lax.rem(x + 1, NX)}
    minus = {X: lax.rem(x + NX - 1, NX)}
    over = {Y: 1 - y}
    mate = {CORE: 1 - k}
    after = {"row": lax.rem(row + 1, rows)}
    before = {"row": lax.rem(row + rows - 1, rows)}

    barrier = pltpu.get_barrier_semaphore()
    for to in (mate, plus, minus, over, after, before):
        pl.semaphore_signal(barrier, inc=1, device_id=to, device_id_type=MESH)

    def load_columns(src, dst, q, which):
        return pltpu.make_async_copy(
            src.at[:, pl.ds(q * G, G)], dst.at[q], load_sem.at[which, q]
        )

    loads = [
        [pltpu.make_async_copy(factor_hbm, factor, factor_sem)],
        [load_columns(back_hbm, cb, q, 0) for q in range(16)],
        [load_columns(in_hbm, ci, q, 1) for q in range(16)],
        [
            pltpu.make_async_copy(
                own_hbm.at[:, :, :, pl.ds(q * G, G)], ibo.at[q], load_sem.at[2, q]
            )
            for q in range(16)
        ],
    ]
    mine = 4 * x + 2 * y + k
    loads[0] += [
        pltpu.make_async_copy(count_hbm.at[row], counts, load_sem.at[3, 0]),
        pltpu.make_async_copy(index_hbm.at[row, mine], index, load_sem.at[3, 1]),
    ]
    def start(load):
        for copy in load:
            copy.start()

    def wait_for(load):
        for copy in load:
            copy.wait()

    start(loads[0])

    def swap(src, dst, n):
        return pltpu.make_async_remote_copy(
            src_ref=src, dst_ref=dst, send_sem=swap_send.at[n], recv_sem=swap_recv.at[n],
            device_id=mate, device_id_type=MESH,
        )

    swaps = {
        "back1": swap(bt.at[pl.ds(8, 8), 1 - k], bp.at[pl.ds(8, 8)], 4),
        "back0": swap(bt.at[pl.ds(0, 8), 1 - k], bp.at[pl.ds(0, 8)], 5),
        "in1": swap(in_o.at[:, pl.ds(1024, 1024)], in_p.at[:, pl.ds(1024, 1024)], 6),
        "in0": swap(in_o.at[:, pl.ds(0, 1024)], in_p.at[:, pl.ds(0, 1024)], 7),
    }
    for block in range(4):
        swaps[block] = swap(ibs.at[block], ibp.at[block], block)

    wait_for(loads[0])
    for load in (loads[3], loads[1], loads[2]):
        start(load)
    n = factor.shape[0]
    at = [index[0, a] for a in range(16)]
    count = counts[mine]
    for p in range(16):
        place = jnp.int32(0)
        for a in range(1, 16):
            place = place + jnp.where(at[a] == p, a, 0)
        tab[0, p] = place & 15
        live[0, p] = jnp.where(place < count, 1.0, 0.0)

    def part(i, j):
        return factor[i * G : (i + 1) * G, j * G : (j + 1) * G]

    x0, x1, x2 = inverses_of_blocks([part(i, i) for i in range(3)])
    x10 = -mm(mm(x1, part(1, 0)), x0)
    t0 = mm(x2, part(2, 0))
    t1 = mm(x2, part(2, 1))
    x20 = -(mm(t0, x0) + mm(t1, x10))
    x21 = -mm(t1, x1)
    zero = jnp.zeros((G, G), jnp.float32)
    for i, line in enumerate(((x0, zero, zero), (x10, x1, zero), (x20, x21, x2))):
        for j, piece in enumerate(line):
            high = piece.astype(jnp.bfloat16)
            w[i * G : (i + 1) * G, j * G : (j + 1) * G] = high
            w[i * G : (i + 1) * G, n + j * G : n + (j + 1) * G] = (
                piece - high.astype(jnp.float32)
            ).astype(jnp.bfloat16)

    def window_granule(h, j):
        return h * 8 + 2 * lax.rem(x + j // 2, NX) + lax.rem(j + y, 2)

    def granule_of(ref, p):
        a = tab[0, p]
        piece = ref[a]
        return piece * jnp.full(piece.shape, live[0, p]).astype(piece.dtype)

    def solve_back(h):
        def body(pair, _):
            pieces = [granule_of(cb, window_granule(h, 2 * pair + i)) for i in (0, 1)]
            both = jnp.concatenate(pieces, axis=1)
            twice = jnp.concatenate([both, both], axis=0)
            solved = lax.dot_general(
                twice, w[...], (((0,), (1,)), ((), ())), preferred_element_type=jnp.float32
            ).astype(jnp.bfloat16)
            bt[pl.ds(h * 8 + 2 * pair, 2)] = solved.reshape(2, 2, 64, n)
            return 0

        lax.fori_loop(0, 4, body, 0, unroll=True)

    def solve_in(half):
        def body(pair, _):
            p = half * 8 + 2 * pair
            both = jnp.concatenate([granule_of(ci, p), granule_of(ci, p + 1)], axis=1)
            twice = jnp.concatenate([both, both], axis=0)
            solved = jnp.dot(w[...], twice, preferred_element_type=jnp.float32)
            in_o[:, pl.ds(pl.multiple_of(p * G, 2 * G), 2 * G)] = solved.astype(jnp.bfloat16)
            return 0

        lax.fori_loop(0, 4, body, 0, unroll=True)

    def gather(block):
        h, half = block // 2, block % 2

        def body(j, _):
            g = window_granule(h, j)
            for q in range(8):
                p = half * 8 + q
                tile = ibo[tab[0, p], tab[0, g], 1 - k]
                keep = jnp.full(tile.shape, live[0, g] * live[0, p]).astype(tile.dtype)
                ibs[block, j, q] = tile * keep
            return 0

        lax.fori_loop(0, 8, body, 0, unroll=2)

    wait_for(loads[3])
    gather(2)
    wait_for(loads[1])
    solve_back(1)
    pl.semaphore_wait(barrier, 6)
    swaps[2].start()
    swaps["back1"].start()
    wait_for(loads[2])
    solve_in(0)
    swaps["in0"].start()
    gather(3)
    swaps[3].start()
    solve_in(1)
    swaps["in1"].start()

    def product(block):
        h, half = block // 2, block % 2
        lhs = jnp.concatenate(
            [bt[pl.ds(h * 8, 8), k].reshape(512, n), bp[pl.ds(h * 8, 8)].reshape(512, n)], axis=1
        )

        def body(pair, _):
            p = half * 8 + 2 * pair
            at = pl.ds(pl.multiple_of(p * G, 2 * G), 2 * G)
            rhs = jnp.concatenate([in_o[:, at], in_p[:, at]], axis=0)
            made = jnp.dot(lhs, rhs, preferred_element_type=jnp.float32)
            for j in range(8):
                g = window_granule(h, j)
                for i in (0, 1):
                    total = -made[j * 64 : (j + 1) * 64, i * G : (i + 1) * G]
                    tile = ibo[tab[0, p + i], tab[0, g], k].astype(jnp.float32)
                    total = total + tile * (live[0, g] * live[0, p + i])
                    total = total + ibp[block, j, 2 * pair + i].astype(jnp.float32)
                    acc[h, j, p + i] = total
            return 0

        lax.fori_loop(0, 4, body, 0, unroll=True)

    def copy_of(block, name, tiles, to):
        u = UNIT[block, name]
        size = pl.ds(0, HEAD + 64 * tiles)
        return pltpu.make_async_remote_copy(
            src_ref=sendb.at[u, size], dst_ref=recvb.at[u, size],
            send_sem=send_sem.at[u], recv_sem=recv_sem.at[u],
            device_id=to, device_id_type=MESH,
        )

    copies = []

    def send(block, name, slots, first, last, to):
        u = UNIT[block, name]
        wide = last - first
        most = jnp.full((HEAD, G), 1e-30, jnp.float32)
        for j in slots:
            seen = jnp.abs(acc[block, j, first:last]).reshape(wide * 4, HEAD, G)
            most = jnp.maximum(most, jnp.max(seen, axis=0))
        power = jnp.ceil(jnp.log2(most) + 0.015)
        scale = jnp.exp2(15.0 - power)
        sendb[u, 0:HEAD] = power.astype(jnp.int32).astype(jnp.int16)
        at = HEAD
        for j in slots:
            codes = acc[block, j, first:last].reshape(wide * 4, HEAD, G) * scale[None]
            codes = jnp.round(codes).astype(jnp.int32).astype(jnp.int16)
            sendb[u, at : at + 64 * wide] = codes.reshape(64 * wide, G)
            at += 64 * wide
        copy = copy_of(block, name, len(slots) * wide, to)
        copy.start()
        copies.append(copy)

    def take(block, name, slots, first, last, to, onto=None):
        u = UNIT[block, name]
        wide = last - first
        copy_of(block, name, len(slots) * wide, to).wait_recv()
        scale = jnp.exp2(recvb[u, 0:HEAD].astype(jnp.float32) - 15.0)
        at = HEAD
        h, first, last = (block, first, last) if onto is None else onto
        for j in slots:
            got = recvb[u, at : at + 64 * wide].astype(jnp.float32).reshape(wide * 4, HEAD, G)
            got = (got * scale[None]).reshape(wide, 64, G)
            acc[h, j, first:last] = acc[h, j, first:last] + got
            at += 64 * wide

    a_to, b_to = Y_FIRST, 16
    a_mid = (3, 4)
    b_mid = (12, 11)

    def b_first(h):
        send(h, "b1p", (4, 5), a_to, b_mid[h], plus)
        send(h, "b1m", (4, 5), b_mid[h], b_to, minus)
        send(h, "b2op", (2, 3), b_mid[h], b_to, plus)
        send(h, "b2om", (6, 7), a_to, b_mid[h], minus)

    def b_second(h):
        take(h, "b1p", (2, 3), a_to, b_mid[h], plus)
        send(h, "b2sp", (2, 3), a_to, b_mid[h], plus)
        take(h, "b1m", (6, 7), b_mid[h], b_to, minus)
        send(h, "b2sm", (6, 7), b_mid[h], b_to, minus)

    def b_third(h):
        take(h, "b2op", (0, 1), b_mid[h], b_to, plus)
        take(h, "b2om", (0, 1), a_to, b_mid[h], minus)
        take(h, "b2sp", (0, 1), a_to, b_mid[h], plus)
        take(h, "b2sm", (0, 1), b_mid[h], b_to, minus)
        send(h, "b3", (1,), a_to, b_to, over)

    def b_last(h):
        take(h, "b3", (0,), a_to, b_to, over)

    def a_first(h, order=(2, 1, 3, 0)):
        for d in order:
            send(h, f"a1_{d}", (2 * d + 1,), 0, a_to, over)

    def a_second(h):
        take(h, "a1_2", (4,), 0, a_to, over)
        send(h, "a2p", (4,), 0, a_mid[h], plus)
        send(h, "a2m", (4,), a_mid[h], a_to, minus)
        take(h, "a1_1", (2,), 0, a_to, over)
        send(h, "a3op", (2,), a_mid[h], a_to, plus)
        take(h, "a1_3", (6,), 0, a_to, over)
        send(h, "a3om", (6,), 0, a_mid[h], minus)

    def a_third(h):
        take(h, "a2p", (2,), 0, a_mid[h], plus)
        send(h, "a3sp", (2,), 0, a_mid[h], plus)
        take(h, "a2m", (6,), a_mid[h], a_to, minus)
        send(h, "a3sm", (6,), a_mid[h], a_to, minus)
        take(h, "a1_0", (0,), 0, a_to, over)

    def a_last(h):
        take(h, "a3op", (0,), a_mid[h], a_to, plus)
        take(h, "a3om", (0,), 0, a_mid[h], minus)
        take(h, "a3sp", (0,), 0, a_mid[h], plus)
        take(h, "a3sm", (0,), a_mid[h], a_to, minus)

    def emit(block):
        h, half = block // 2, block % 2
        for q in range(8):
            out[block, :, q * G : (q + 1) * G] = acc[h, 0, half * 8 + q]

    swaps[2].wait_recv()
    swaps["back1"].wait_recv()
    swaps["in0"].wait_recv()
    product(2)
    a_first(1)
    swaps["in1"].wait_recv()
    swaps[3].wait_recv()
    product(3)
    b_first(1)
    gather(0)
    swaps[0].start()
    solve_back(0)
    swaps["back0"].start()
    gather(1)
    swaps[1].start()
    b_second(1)
    swaps["back0"].wait_recv()
    swaps[0].wait_recv()
    product(0)
    a_first(0, (2,))
    a_second(1)
    b_third(1)
    a_first(0, (1, 3, 0))
    swaps[1].wait_recv()
    product(1)
    b_first(0)
    b_last(1)
    send(1, "carry", (0,), 8, 16, after)
    a_third(1)
    b_second(0)
    a_second(0)
    a_last(1)
    emit(2)
    b_third(0)
    a_third(0)
    b_last(0)
    emit(1)
    a_last(0)
    take(1, "carry", (0,), 8, 16, after, onto=(0, 0, 8))
    emit(0)

    for copy in swaps.values():
        copy.wait_send()
    for copy in copies:
        copy.wait_send()


def on_device(interior_factor, coupling_in, coupling_back, interface_block, gran_count, gran_index):
    factor = interior_factor[0, 0, 0]
    inner = coupling_in[0, 0, 0]
    back = coupling_back[0, 0, 0]
    n, width = inner.shape
    own = interface_block[0, 0, 0].reshape(16, 2, 64, width)
    units = len(UNIT)
    size = HEAD + 64 * 10
    hbm = pl.BlockSpec(memory_space=pl.ANY)
    out = pl.pallas_call(
        kernel,
        out_shape=pltpu.VMEM((3, 64, width // 2), jnp.float32),
        in_specs=[hbm, hbm, hbm, hbm, hbm, hbm],
        out_specs=pl.BlockSpec(memory_space=pltpu.VMEM),
        scratch_shapes=[
            pltpu.SMEM((16,), jnp.int32),
            pltpu.SMEM((1, 16), jnp.int32),
            pltpu.SMEM((1, 16), jnp.int32),
            pltpu.SMEM((1, 16), jnp.float32),
            pltpu.VMEM((n, n), jnp.float32),
            pltpu.VMEM((16, n, G), jnp.bfloat16),
            pltpu.VMEM((16, n, G), jnp.bfloat16),
            pltpu.VMEM((16, 16, 2, 64, G), jnp.bfloat16),
            pltpu.VMEM((4, 8, 8, 64, G), jnp.bfloat16),
            pltpu.VMEM((4, 8, 8, 64, G), jnp.bfloat16),
            pltpu.VMEM((n, 2 * n), jnp.bfloat16),
            pltpu.VMEM((n, width), jnp.bfloat16),
            pltpu.VMEM((n, width), jnp.bfloat16),
            pltpu.VMEM((16, 2, 64, n), jnp.bfloat16),
            pltpu.VMEM((16, 64, n), jnp.bfloat16),
            pltpu.VMEM((2, 8, 16, 64, G), jnp.float32),
            pltpu.VMEM((units, size, G), jnp.int16),
            pltpu.VMEM((units, size, G), jnp.int16),
            pltpu.SemaphoreType.DMA,
            pltpu.SemaphoreType.DMA((4, 16)),
            pltpu.SemaphoreType.DMA((8,)),
            pltpu.SemaphoreType.DMA((8,)),
            pltpu.SemaphoreType.DMA((units,)),
            pltpu.SemaphoreType.DMA((units,)),
        ],
        compiler_params=pltpu.CompilerParams(
            collective_id=0, has_side_effects=True, vmem_limit_bytes=56 * 1024 * 1024
        ),
    )(gran_count[:, :, 0], gran_index, factor, inner, back, own)
    return out[None]


def solution(mesh):
    split = Mesh(mesh.devices.reshape(mesh.shape["row"], 4, 2, 2), ("row", X, Y, CORE))
    spec = P("row", COL, None, None, None)
    return jax.shard_map(
        on_device,
        mesh=split,
        in_specs=(spec, spec, spec, spec, P(), P()),
        out_specs=P("row", None, COL, None),
        check_vma=False,
    )
```

```python
import functools

import jax
import jax.numpy as jnp
from jax import lax
from jax.experimental import pallas as pl
from jax.experimental.pallas import tpu as pltpu
from jax.sharding import Mesh
from jax.sharding import PartitionSpec as P

MESH = pl.DeviceIdType.MESH
X, Y, CORE = "col_0", "col_1", "col_2"
COL = (X, Y, CORE)
NX = 4
G = 128
HEAD = 16
HIGHEST = lax.Precision.HIGHEST

Y_FIRST = 7
B_UNITS = ["b1p", "b1m", "b2op", "b2om", "b2sp", "b2sm", "b3"]
A_UNITS = ["a1_2", "a1_1", "a1_3", "a1_0", "a2p", "a2m", "a3op", "a3om", "a3sp", "a3sm"]


def unit_numbers():
    names = [(h, u) for h in (1, 0) for u in B_UNITS + A_UNITS] + [(1, "carry")]
    return {name: i for i, name in enumerate(names)}


UNIT = unit_numbers()


def mm(a, b):
    return jnp.dot(a, b, precision=HIGHEST, preferred_element_type=jnp.float32)


def inverses_of_blocks(blocks):
    n = blocks[0].shape[0]
    row = lax.broadcasted_iota(jnp.int32, (n, n), 0)
    col = lax.broadcasted_iota(jnp.int32, (n, n), 1)

    def below(shift):
        upper, lower = row >> shift, col >> shift
        return ((upper & 1) == 1) & (upper == lower + 1)

    found = []
    for block in blocks:
        diagonal = jnp.where(row == col, block, 0.0)
        down = 1.0 / jnp.sum(diagonal, axis=1, keepdims=True)
        across = 1.0 / jnp.sum(diagonal, axis=0, keepdims=True)
        under = jnp.where(below(0), block, 0.0)
        found.append(jnp.where(row == col, down, 0.0) - under * down * across)
    for shift in range(1, 7):
        mask = below(shift)
        lines = [mm(f, jnp.where(mask, block, 0.0)) for f, block in zip(found, blocks)]
        found = [f - mm(line, f) for f, line in zip(found, lines)]
    return found


def kernel(
    count_hbm, index_hbm, factor_hbm, in_hbm, back_hbm, own_hbm, out,
    counts, index, tab, live, factor, ci, cb, ibo, ibs, ibp, w, in_o, in_p, bt, bp, acc, sendb, recvb,
    factor_sem, load_sem, swap_send, swap_recv, send_sem, recv_sem,
):
    row = lax.axis_index("row")
    rows = lax.axis_size("row")
    x = lax.axis_index(X)
    y = lax.axis_index(Y)
    k = lax.axis_index(CORE)
    plus = {X: lax.rem(x + 1, NX)}
    minus = {X: lax.rem(x + NX - 1, NX)}
    over = {Y: 1 - y}
    mate = {CORE: 1 - k}
    after = {"row": lax.rem(row + 1, rows)}
    before = {"row": lax.rem(row + rows - 1, rows)}

    barrier = pltpu.get_barrier_semaphore()
    for to in (mate, plus, minus, over, after, before):
        pl.semaphore_signal(barrier, inc=1, device_id=to, device_id_type=MESH)

    def load_columns(src, dst, q, which):
        return pltpu.make_async_copy(
            src.at[:, pl.ds(q * G, G)], dst.at[q], load_sem.at[which, q]
        )

    loads = [
        [pltpu.make_async_copy(factor_hbm, factor, factor_sem)],
        [load_columns(back_hbm, cb, q, 0) for q in range(16)],
        [load_columns(in_hbm, ci, q, 1) for q in range(16)],
        [
            pltpu.make_async_copy(
                own_hbm.at[:, :, :, pl.ds(q * G, G)], ibo.at[q], load_sem.at[2, q]
            )
            for q in range(16)
        ],
    ]
    mine = 4 * x + 2 * y + k
    loads[0] += [
        pltpu.make_async_copy(count_hbm.at[row], counts, load_sem.at[3, 0]),
        pltpu.make_async_copy(index_hbm.at[row, mine], index, load_sem.at[3, 1]),
    ]
    def start(load):
        for copy in load:
            copy.start()

    def wait_for(load):
        for copy in load:
            copy.wait()

    start(loads[0])

    def swap(src, dst, n):
        return pltpu.make_async_remote_copy(
            src_ref=src, dst_ref=dst, send_sem=swap_send.at[n], recv_sem=swap_recv.at[n],
            device_id=mate, device_id_type=MESH,
        )

    swaps = {
        "back1": swap(bt.at[pl.ds(8, 8), 1 - k], bp.at[pl.ds(8, 8)], 4),
        "back0": swap(bt.at[pl.ds(0, 8), 1 - k], bp.at[pl.ds(0, 8)], 5),
        "in1": swap(in_o.at[:, pl.ds(1024, 1024)], in_p.at[:, pl.ds(1024, 1024)], 6),
        "in0": swap(in_o.at[:, pl.ds(0, 1024)], in_p.at[:, pl.ds(0, 1024)], 7),
    }
    for block in range(4):
        swaps[block] = swap(ibs.at[block], ibp.at[block], block)

    wait_for(loads[0])
    for load in (loads[3], loads[1], loads[2]):
        start(load)
    n = factor.shape[0]
    at = [index[0, a] for a in range(16)]
    count = counts[mine]
    for p in range(16):
        place = jnp.int32(0)
        for a in range(1, 16):
            place = place + jnp.where(at[a] == p, a, 0)
        tab[0, p] = place & 15
        live[0, p] = jnp.where(place < count, 1.0, 0.0)

    def part(i, j):
        return factor[i * G : (i + 1) * G, j * G : (j + 1) * G]

    x0, x1, x2 = inverses_of_blocks([part(i, i) for i in range(3)])
    x10 = -mm(mm(x1, part(1, 0)), x0)
    t0 = mm(x2, part(2, 0))
    t1 = mm(x2, part(2, 1))
    x20 = -(mm(t0, x0) + mm(t1, x10))
    x21 = -mm(t1, x1)
    zero = jnp.zeros((G, G), jnp.float32)
    for i, line in enumerate(((x0, zero, zero), (x10, x1, zero), (x20, x21, x2))):
        for j, piece in enumerate(line):
            high = piece.astype(jnp.bfloat16)
            w[i * G : (i + 1) * G, j * G : (j + 1) * G] = high
            w[i * G : (i + 1) * G, n + j * G : n + (j + 1) * G] = (
                piece - high.astype(jnp.float32)
            ).astype(jnp.bfloat16)

    def window_granule(h, j):
        return h * 8 + 2 * lax.rem(x + j // 2, NX) + lax.rem(j + y, 2)

    def granule_of(ref, p):
        a = tab[0, p]
        piece = ref[a]
        return piece * jnp.full(piece.shape, live[0, p]).astype(piece.dtype)

    def solve_back(h):
        def body(pair, _):
            pieces = [granule_of(cb, window_granule(h, 2 * pair + i)) for i in (0, 1)]
            both = jnp.concatenate(pieces, axis=1)
            twice = jnp.concatenate([both, both], axis=0)
            solved = lax.dot_general(
                twice, w[...], (((0,), (1,)), ((), ())), preferred_element_type=jnp.float32
            ).astype(jnp.bfloat16)
            bt[pl.ds(h * 8 + 2 * pair, 2)] = solved.reshape(2, 2, 64, n)
            return 0

        lax.fori_loop(0, 4, body, 0, unroll=True)

    def solve_in(half):
        def body(pair, _):
            p = half * 8 + 2 * pair
            both = jnp.concatenate([granule_of(ci, p), granule_of(ci, p + 1)], axis=1)
            twice = jnp.concatenate([both, both], axis=0)
            solved = jnp.dot(w[...], twice, preferred_element_type=jnp.float32)
            in_o[:, pl.ds(pl.multiple_of(p * G, 2 * G), 2 * G)] = solved.astype(jnp.bfloat16)
            return 0

        lax.fori_loop(0, 4, body, 0, unroll=True)

    def gather(block):
        h, half = block // 2, block % 2

        def body(j, _):
            g = window_granule(h, j)
            for q in range(8):
                p = half * 8 + q
                tile = ibo[tab[0, p], tab[0, g], 1 - k]
                keep = jnp.full(tile.shape, live[0, g] * live[0, p]).astype(tile.dtype)
                ibs[block, j, q] = tile * keep
            return 0

        lax.fori_loop(0, 8, body, 0, unroll=2)

    wait_for(loads[3])
    gather(2)
    wait_for(loads[1])
    solve_back(1)
    pl.semaphore_wait(barrier, 6)
    swaps[2].start()
    swaps["back1"].start()
    wait_for(loads[2])
    solve_in(0)
    swaps["in0"].start()
    gather(3)
    swaps[3].start()
    solve_in(1)
    swaps["in1"].start()

    def product(block, part):
        h, half = block // 2, block % 2
        line = 8 * h + 4 * part
        lhs = jnp.concatenate(
            [bt[pl.ds(line, 4), k].reshape(256, n), bp[pl.ds(line, 4)].reshape(256, n)], axis=1
        )

        def body(pair, _):
            p = half * 8 + 2 * pair
            at = pl.ds(pl.multiple_of(p * G, 2 * G), 2 * G)
            rhs = jnp.concatenate([in_o[:, at], in_p[:, at]], axis=0)
            made = jnp.dot(lhs, rhs, preferred_element_type=jnp.float32)
            for j in range(4 * part, 4 * part + 4):
                g = window_granule(h, j)
                for i in (0, 1):
                    at_row = (j - 4 * part) * 64
                    total = -made[at_row : at_row + 64, i * G : (i + 1) * G]
                    tile = ibo[tab[0, p + i], tab[0, g], k].astype(jnp.float32)
                    total = total + tile * (live[0, g] * live[0, p + i])
                    total = total + ibp[block, j, 2 * pair + i].astype(jnp.float32)
                    acc[h, j, p + i] = total
            return 0

        lax.fori_loop(0, 4, body, 0, unroll=True)

    def copy_of(block, name, tiles, to):
        u = UNIT[block, name]
        size = pl.ds(0, HEAD + 64 * tiles)
        return pltpu.make_async_remote_copy(
            src_ref=sendb.at[u, size], dst_ref=recvb.at[u, size],
            send_sem=send_sem.at[u], recv_sem=recv_sem.at[u],
            device_id=to, device_id_type=MESH,
        )

    copies = []

    def send(block, name, slots, first, last, to):
        u = UNIT[block, name]
        wide = last - first
        most = jnp.full((HEAD, G), 1e-30, jnp.float32)
        for j in slots:
            seen = jnp.abs(acc[block, j, first:last]).reshape(wide * 4, HEAD, G)
            most = jnp.maximum(most, jnp.max(seen, axis=0))
        power = jnp.ceil(jnp.log2(most) + 0.015)
        scale = jnp.exp2(15.0 - power)
        sendb[u, 0:HEAD] = power.astype(jnp.int32).astype(jnp.int16)
        at = HEAD
        for j in slots:
            codes = acc[block, j, first:last].reshape(wide * 4, HEAD, G) * scale[None]
            codes = jnp.round(codes).astype(jnp.int32).astype(jnp.int16)
            sendb[u, at : at + 64 * wide] = codes.reshape(64 * wide, G)
            at += 64 * wide
        copy = copy_of(block, name, len(slots) * wide, to)
        copy.start()
        copies.append(copy)

    def take(block, name, slots, first, last, to, onto=None):
        u = UNIT[block, name]
        wide = last - first
        copy_of(block, name, len(slots) * wide, to).wait_recv()
        scale = jnp.exp2(recvb[u, 0:HEAD].astype(jnp.float32) - 15.0)
        at = HEAD
        h, first, last = (block, first, last) if onto is None else onto
        for j in slots:
            got = recvb[u, at : at + 64 * wide].astype(jnp.float32).reshape(wide * 4, HEAD, G)
            got = (got * scale[None]).reshape(wide, 64, G)
            acc[h, j, first:last] = acc[h, j, first:last] + got
            at += 64 * wide

    a_to, b_to = Y_FIRST, 16
    a_mid = (3, 4)
    b_mid = (12, 11)

    def b_first(h):
        send(h, "b1p", (4, 5), a_to, b_mid[h], plus)
        send(h, "b1m", (4, 5), b_mid[h], b_to, minus)
        send(h, "b2om", (6, 7), a_to, b_mid[h], minus)

    def b_direct(h):
        send(h, "b2op", (2, 3), b_mid[h], b_to, plus)

    def b_second(h):
        take(h, "b1p", (2, 3), a_to, b_mid[h], plus)
        send(h, "b2sp", (2, 3), a_to, b_mid[h], plus)
        take(h, "b1m", (6, 7), b_mid[h], b_to, minus)
        send(h, "b2sm", (6, 7), b_mid[h], b_to, minus)

    def b_third(h):
        take(h, "b2op", (0, 1), b_mid[h], b_to, plus)
        take(h, "b2om", (0, 1), a_to, b_mid[h], minus)
        take(h, "b2sp", (0, 1), a_to, b_mid[h], plus)
        take(h, "b2sm", (0, 1), b_mid[h], b_to, minus)
        send(h, "b3", (1,), a_to, b_to, over)

    def b_last(h):
        take(h, "b3", (0,), a_to, b_to, over)

    def a_first(h, order=(2, 1, 3, 0)):
        for d in order:
            send(h, f"a1_{d}", (2 * d + 1,), 0, a_to, over)

    def a_second(h):
        take(h, "a1_2", (4,), 0, a_to, over)
        send(h, "a2p", (4,), 0, a_mid[h], plus)
        send(h, "a2m", (4,), a_mid[h], a_to, minus)
        take(h, "a1_1", (2,), 0, a_to, over)
        send(h, "a3op", (2,), a_mid[h], a_to, plus)
        take(h, "a1_3", (6,), 0, a_to, over)
        send(h, "a3om", (6,), 0, a_mid[h], minus)

    def a_third(h):
        take(h, "a2p", (2,), 0, a_mid[h], plus)
        send(h, "a3sp", (2,), 0, a_mid[h], plus)
        take(h, "a2m", (6,), a_mid[h], a_to, minus)
        send(h, "a3sm", (6,), a_mid[h], a_to, minus)
        take(h, "a1_0", (0,), 0, a_to, over)

    def a_last(h):
        take(h, "a3op", (0,), a_mid[h], a_to, plus)
        take(h, "a3om", (0,), 0, a_mid[h], minus)
        take(h, "a3sp", (0,), 0, a_mid[h], plus)
        take(h, "a3sm", (0,), a_mid[h], a_to, minus)

    def emit(block):
        h, half = block // 2, block % 2
        for q in range(8):
            out[block, :, q * G : (q + 1) * G] = acc[h, 0, half * 8 + q]

    swaps[2].wait_recv()
    swaps["back1"].wait_recv()
    swaps["in0"].wait_recv()
    product(2, 1)
    a_first(1, (2, 3))
    product(2, 0)
    a_first(1, (1, 0))
    swaps["in1"].wait_recv()
    swaps[3].wait_recv()
    product(3, 1)
    b_first(1)
    product(3, 0)
    b_direct(1)
    gather(0)
    swaps[0].start()
    solve_back(0)
    swaps["back0"].start()
    gather(1)
    swaps[1].start()
    b_second(1)
    swaps["back0"].wait_recv()
    swaps[0].wait_recv()
    product(0, 1)
    product(0, 0)
    a_first(0, (2,))
    a_second(1)
    b_third(1)
    a_first(0, (1, 3, 0))
    swaps[1].wait_recv()
    product(1, 1)
    b_first(0)
    product(1, 0)
    b_direct(0)
    b_last(1)
    send(1, "carry", (0,), 8, 16, after)
    b_second(0)
    a_third(1)
    a_second(0)
    b_third(0)
    a_last(1)
    emit(2)
    a_third(0)
    b_last(0)
    emit(1)
    a_last(0)
    take(1, "carry", (0,), 8, 16, after, onto=(0, 0, 8))
    emit(0)

    for copy in swaps.values():
        copy.wait_send()
    for copy in copies:
        copy.wait_send()


def on_device(interior_factor, coupling_in, coupling_back, interface_block, gran_count, gran_index):
    factor = interior_factor[0, 0, 0]
    inner = coupling_in[0, 0, 0]
    back = coupling_back[0, 0, 0]
    n, width = inner.shape
    own = interface_block[0, 0, 0].reshape(16, 2, 64, width)
    units = len(UNIT)
    size = HEAD + 64 * 10
    hbm = pl.BlockSpec(memory_space=pl.ANY)
    out = pl.pallas_call(
        kernel,
        out_shape=pltpu.VMEM((3, 64, width // 2), jnp.float32),
        in_specs=[hbm, hbm, hbm, hbm, hbm, hbm],
        out_specs=pl.BlockSpec(memory_space=pltpu.VMEM),
        scratch_shapes=[
            pltpu.SMEM((16,), jnp.int32),
            pltpu.SMEM((1, 16), jnp.int32),
            pltpu.SMEM((1, 16), jnp.int32),
            pltpu.SMEM((1, 16), jnp.float32),
            pltpu.VMEM((n, n), jnp.float32),
            pltpu.VMEM((16, n, G), jnp.bfloat16),
            pltpu.VMEM((16, n, G), jnp.bfloat16),
            pltpu.VMEM((16, 16, 2, 64, G), jnp.bfloat16),
            pltpu.VMEM((4, 8, 8, 64, G), jnp.bfloat16),
            pltpu.VMEM((4, 8, 8, 64, G), jnp.bfloat16),
            pltpu.VMEM((n, 2 * n), jnp.bfloat16),
            pltpu.VMEM((n, width), jnp.bfloat16),
            pltpu.VMEM((n, width), jnp.bfloat16),
            pltpu.VMEM((16, 2, 64, n), jnp.bfloat16),
            pltpu.VMEM((16, 64, n), jnp.bfloat16),
            pltpu.VMEM((2, 8, 16, 64, G), jnp.float32),
            pltpu.VMEM((units, size, G), jnp.int16),
            pltpu.VMEM((units, size, G), jnp.int16),
            pltpu.SemaphoreType.DMA,
            pltpu.SemaphoreType.DMA((4, 16)),
            pltpu.SemaphoreType.DMA((8,)),
            pltpu.SemaphoreType.DMA((8,)),
            pltpu.SemaphoreType.DMA((units,)),
            pltpu.SemaphoreType.DMA((units,)),
        ],
        compiler_params=pltpu.CompilerParams(
            collective_id=0, has_side_effects=True, vmem_limit_bytes=56 * 1024 * 1024
        ),
    )(gran_count[:, :, 0], gran_index, factor, inner, back, own)
    return out[None]


def solution(mesh):
    split = Mesh(mesh.devices.reshape(mesh.shape["row"], 4, 2, 2), ("row", X, Y, CORE))
    spec = P("row", COL, None, None, None)
    return jax.shard_map(
        on_device,
        mesh=split,
        in_specs=(spec, spec, spec, spec, P(), P()),
        out_specs=P("row", None, COL, None),
        check_vma=False,
    )
```
